32 devices in a mesh: gx: 4 (over y, x), gy: 2 (over core), gz: 4 (over z).
Axes of the slice: x: 2, y: 2, z: 4, core: 2. Of those that a mesh axis runs over, the one named last changes fastest.
Arguments:
- conserved: float32 [5, 64, 32, 512], P(None, 'gx', 'gy', 'gz'), as said below
Outputs:
- advanced: float32 [5, 64, 32, 512], P(None, 'gx', 'gy', 'gz')
Inputs may be any that keep to these rules, and one draw needn't show every extreme that they name: `conserved`: every cell has positive density and positive pressure (energy above the kinetic energy).
All inputs are finite; a program needn't handle non-finite values. Where the reference program divides by a largest or mean magnitude, that divisor is 1e-20 or more.
Results may differ from the reference program's by a relative error of at most 0.000066.
Values sent between devices are 32-bit elements; how exact they have to be, the bound alone decides.
A program may use at most 64 MiB of HBM per device.

```python
import jax
import jax.numpy as jnp
from jax import lax

NX = 64
NY = 32
NZ = 512


def draw_conserved(key, part):
    subkeys = jax.random.split(key, 3)
    grid_shape = (NX, NY, NZ)
    log_density = jax.random.uniform(subkeys[0], grid_shape, jnp.float32, -0.7, 0.7)
    log_pressure = jax.random.uniform(subkeys[1], grid_shape, jnp.float32, -0.7, 0.7)
    position = jnp.arange(NX, dtype=jnp.float32) / NX
    vel_scale = (0.3 + 0.6 * position)[:, None, None]
    velocity = jax.random.truncated_normal(subkeys[2], -4.0, 4.0, (3,) + grid_shape, jnp.float32) * vel_scale
    density = jnp.exp(log_density)
    pressure = jnp.exp(log_pressure)
    momentum = density * velocity
    energy = pressure / 0.4 + 0.5 * density * jnp.sum(velocity * velocity, axis=0)
    return jnp.stack([density, momentum[0], momentum[1], momentum[2], energy]).astype(jnp.float32)


def setup_inputs(seed: int = 0) -> dict:
    key_list = jax.random.split(jax.random.key(seed), 2)
    return {
        "conserved": draw_conserved(jax.random.fold_in(key_list[1], 71), 0),
    }


gamma_gas = 1.4
weno_eps = 1e-06
courant = 0.4

def primitives(components):
    density = components[0]
    vel_normal = components[1] / density
    vel_first = components[2] / density
    vel_second = components[3] / density
    kinetic = 0.5 * (vel_normal * vel_normal + vel_first * vel_first + vel_second * vel_second)
    pressure = (gamma_gas - 1.0) * (components[4] - density * kinetic)
    return (density, vel_normal, vel_first, vel_second, kinetic, pressure)

def multiply_rows(matrix, vector):
    result = []
    for matrix_row in matrix:
        accum = None
        for coefficient, component in zip(matrix_row, vector):
            if coefficient is None:
                continue
            product_term = component * coefficient
            accum = product_term if accum is None else accum + product_term
        result.append(accum)
    return result

def weno_face(far_left, near_left, centre, near_right, far_right):
    poly_left = (2.0 * far_left - 7.0 * near_left + 11.0 * centre) / 6.0
    poly_mid = (-near_left + 5.0 * centre + 2.0 * near_right) / 6.0
    poly_right = (2.0 * centre + 5.0 * near_right - far_right) / 6.0
    diff_one = far_left - 2.0 * near_left + centre
    diff_two = far_left - 4.0 * near_left + 3.0 * centre
    smooth_left = 13.0 / 12.0 * diff_one * diff_one + 0.25 * diff_two * diff_two
    diff_one = near_left - 2.0 * centre + near_right
    diff_two = near_left - near_right
    smooth_mid = 13.0 / 12.0 * diff_one * diff_one + 0.25 * diff_two * diff_two
    diff_one = centre - 2.0 * near_right + far_right
    diff_two = 3.0 * centre - 4.0 * near_right + far_right
    smooth_right = 13.0 / 12.0 * diff_one * diff_one + 0.25 * diff_two * diff_two
    weight_left = 0.1 / ((weno_eps + smooth_left) * (weno_eps + smooth_left))
    weight_mid = 0.6 / ((weno_eps + smooth_mid) * (weno_eps + smooth_mid))
    weight_right = 0.3 / ((weno_eps + smooth_right) * (weno_eps + smooth_right))
    return (weight_left * poly_left + weight_mid * poly_mid + weight_right * poly_right) / (weight_left + weight_mid + weight_right)

def face_divergence(components, line_axis, wave_speed, cell_count):
    length = components[0].shape[line_axis] - 6
    face_count = length + 1

    def window(array_item, start, count):
        return lax.slice_in_dim(array_item, start, start + count, axis=line_axis)
    density, vel_normal, vel_first, vel_second, kinetic, pressure = primitives(components)
    fluxes = [components[1], components[1] * vel_normal + pressure, components[2] * vel_normal, components[3] * vel_normal, (components[4] + pressure) * vel_normal]
    split_plus = [0.5 * (flux + wave_speed * component) for flux, component in zip(fluxes, components)]
    split_minus = [0.5 * (flux - wave_speed * component) for flux, component in zip(fluxes, components)]
    face_mean = [0.5 * (window(component, 2, face_count) + window(component, 3, face_count)) for component in components]
    mean_density, mean_normal, mean_first, mean_second, mean_kinetic, mean_pressure = primitives(face_mean)
    enthalpy = (face_mean[4] + mean_pressure) / mean_density
    sound_speed = jnp.sqrt(gamma_gas * mean_pressure / mean_density)
    inv_sound = 1.0 / sound_speed
    coef_one = (gamma_gas - 1.0) / (sound_speed * sound_speed)
    coef_two = coef_one * mean_kinetic
    left_rows = [[0.5 * (coef_two + mean_normal * inv_sound), -0.5 * (coef_one * mean_normal + inv_sound), -0.5 * coef_one * mean_first, -0.5 * coef_one * mean_second, 0.5 * coef_one], [-mean_first, None, 1.0, None, None], [-mean_second, None, None, 1.0, None], [1.0 - coef_two, coef_one * mean_normal, coef_one * mean_first, coef_one * mean_second, -coef_one], [0.5 * (coef_two - mean_normal * inv_sound), -0.5 * (coef_one * mean_normal - inv_sound), -0.5 * coef_one * mean_first, -0.5 * coef_one * mean_second, 0.5 * coef_one]]
    right_cols = [[1.0, None, None, 1.0, 1.0], [mean_normal - sound_speed, None, None, mean_normal, mean_normal + sound_speed], [mean_first, 1.0, None, mean_first, mean_first], [mean_second, None, 1.0, mean_second, mean_second], [enthalpy - mean_normal * sound_speed, mean_first, mean_second, mean_kinetic, enthalpy + mean_normal * sound_speed]]
    positive = [multiply_rows(left_rows, [window(component, offset, face_count) for component in split_plus]) for offset in range(5)]
    negative = [multiply_rows(left_rows, [window(component, offset, face_count) for component in split_minus]) for offset in range(1, 6)]
    wave_sums = []
    for wave_index in range(5):
        upwind = weno_face(*[positive[offset][wave_index] for offset in range(5)])
        downwind = weno_face(*[negative[offset][wave_index] for offset in (4, 3, 2, 1, 0)])
        wave_sums.append(upwind + downwind)
    face_flux = multiply_rows(right_cols, wave_sums)
    return [-(window(flux, 1, length) - window(flux, 0, length)) * cell_count for flux in face_flux]

def component_order(direction):
    if direction == 0:
        return [0, 1, 2, 3, 4]
    if direction == 1:
        return [0, 2, 1, 3, 4]
    return [0, 3, 1, 2, 4]

def direction_terms(padded_slab, line_axis, direction, wave_speed, cell_count):
    comp_order = component_order(direction)
    result = face_divergence([padded_slab[index] for index in comp_order], line_axis, wave_speed, cell_count)
    placed = [None] * 5
    for index, target in enumerate(comp_order):
        placed[target] = result[index]
    return jnp.stack(placed)

def reference(conserved):
    components = [conserved[index] for index in range(5)]
    density, vel_one, vel_two, vel_three, kinetic, pressure = primitives(components)
    sound_speed = jnp.sqrt(gamma_gas * pressure / density)
    speed_x = jnp.max(jnp.abs(vel_one) + sound_speed)
    speed_y = jnp.max(jnp.abs(vel_two) + sound_speed)
    speed_z = jnp.max(jnp.abs(vel_three) + sound_speed)
    step = courant / (speed_x * NX + speed_y * NY + speed_z * NZ)
    padded = jnp.pad(conserved, ((0, 0), (3, 3), (0, 0), (0, 0)), mode='wrap')
    moved = jnp.moveaxis(padded, 2, 0)
    result = lax.map(lambda slab_item: direction_terms(slab_item, 0, 0, speed_x, NX), moved)
    tendency = jnp.moveaxis(result, 0, 2)
    padded = jnp.pad(conserved, ((0, 0), (0, 0), (3, 3), (0, 0)), mode='wrap')
    moved = jnp.moveaxis(padded, 1, 0)
    result = lax.map(lambda slab_item: direction_terms(slab_item, 0, 1, speed_y, NY), moved)
    tendency = tendency + jnp.moveaxis(result, 0, 1)
    padded = jnp.pad(conserved, ((0, 0), (0, 0), (0, 0), (3, 3)), mode='wrap')
    moved = jnp.moveaxis(padded, 1, 0)
    result = lax.map(lambda slab_item: direction_terms(slab_item, 1, 2, speed_z, NZ), moved)
    tendency = tendency + jnp.moveaxis(result, 0, 1)
    return conserved + step * tendency
```

```python
import functools

import jax
import jax.numpy as jnp
from jax import lax
from jax.experimental import pallas as pl
from jax.experimental.pallas import tpu as pltpu
from jax.sharding import PartitionSpec as P

GAMMA = 1.4
EPS = 1e-06
COURANT = 0.4
K13 = 13.0 / 3.0
MESH = pl.DeviceIdType.MESH
AXES = ("gx", "gy", "gz")
ORDERS = ([0, 1, 2, 3, 4], [0, 2, 1, 3, 4], [0, 3, 1, 2, 4])
LANES = 128


def exchange_kernel(
    sizes, shape, cons, xh, yh, zh, zt, top, ysend, zsend, mine, theirs,
    halo_send, halo_recv, max_send, max_recv,
):
    lx, ly, lz = shape
    rows = lx * ly
    groups = rows // LANES
    blocks = 8 // groups
    inner = lz // blocks
    peers = []
    for axis, size in zip(AXES, sizes):
        me = lax.axis_index(axis)
        peers.append([{axis: lax.rem(me + k, size)} for k in range(1, size)])
    barrier = pltpu.get_barrier_semaphore()
    count = 0
    for axis_peers in peers:
        for peer in axis_peers:
            pl.semaphore_signal(barrier, inc=1, device_id=peer, device_id_type=MESH)
            count += 1

    best = [None] * 3
    for j in range(rows // 8):
        q = [cons[c, pl.ds(8 * j, 8), :] for c in range(5)]
        inv = 1.0 / q[0]
        vel = [q[d] * inv for d in (1, 2, 3)]
        kinetic = 0.5 * (vel[0] * vel[0] + vel[1] * vel[1] + vel[2] * vel[2])
        sound = jnp.sqrt((GAMMA * (GAMMA - 1.0)) * (q[4] * inv - kinetic))
        for d in range(3):
            value = jnp.abs(vel[d]) + sound
            best[d] = value if best[d] is None else jnp.maximum(best[d], value)
    for d in range(3):
        mine[0, pl.ds(8 * d, 8), :] = best[d]

    for c in range(5):
        for k in range(3):
            ysend[0, c, pl.ds(k * lx, lx), :] = cons[c, pl.ds(ly - 3 + k, lx, stride=ly), :]
            ysend[1, c, pl.ds(k * lx, lx), :] = cons[c, pl.ds(k, lx, stride=ly), :]

    def halo(slot, src, dst, axis, size, up):
        me = lax.axis_index(axis)
        target = lax.rem(me + (1 if up else size - 1), size)
        return pltpu.make_async_remote_copy(
            src_ref=src, dst_ref=dst, send_sem=halo_send.at[slot], recv_sem=halo_recv.at[slot],
            device_id={axis: target}, device_id_type=MESH,
        )

    def spread(stage):
        axis, size = AXES[stage], sizes[stage]
        copies = []
        for k in range(size - 1):
            slot = sum(s - 1 for s in sizes[:stage]) + k
            copy = pltpu.make_async_remote_copy(
                src_ref=mine.at[position[stage]], dst_ref=theirs.at[slot],
                send_sem=max_send.at[slot], recv_sem=max_recv.at[slot],
                device_id=peers[stage][k], device_id_type=MESH,
            )
            copy.start()
            copies.append((slot, copy))
        return copies

    def gather(stage, copies):
        value = mine[position[stage]]
        for slot, copy in copies:
            copy.wait_recv()
            value = jnp.maximum(value, theirs[slot])
        return value

    order = (1, 2, 0)
    position = {stage: place for place, stage in enumerate(order)}
    started = []
    pl.semaphore_wait(barrier, count)
    copies = spread(order[0])
    started += copies
    edge = 3 * ly
    halos = [
        halo(0, cons.at[:, pl.ds(rows - edge, edge), :], xh.at[0], "gx", sizes[0], True),
        halo(1, cons.at[:, pl.ds(0, edge), :], xh.at[1], "gx", sizes[0], False),
        halo(2, ysend.at[0], yh.at[0], "gy", sizes[1], True),
        halo(3, ysend.at[1], yh.at[1], "gy", sizes[1], False),
    ]
    value = gather(order[0], copies)
    mine[1] = value
    copies = spread(order[1])
    started += copies
    for copy in halos:
        copy.start()

    for c in range(5):
        for g in range(groups):
            turned = jnp.transpose(cons[c, pl.ds(g * LANES, LANES), :])
            for b in range(blocks):
                zt[c, pl.ds(b * groups + g, inner, stride=8), :] = turned[b * inner:(b + 1) * inner]
                if b == blocks - 1:
                    for k in range(3):
                        zsend[0, c, k, g:g + 1, :] = turned[lz - 3 + k:lz - 2 + k]
                if b == 0:
                    for k in range(3):
                        zsend[1, c, k, g:g + 1, :] = turned[k:k + 1]

    value = gather(order[1], copies)
    mine[2] = value
    copies = spread(order[2])
    started += copies
    more = [
        halo(4, zsend.at[0], zh.at[0], "gz", sizes[2], True),
        halo(5, zsend.at[1], zh.at[1], "gz", sizes[2], False),
    ]
    for copy in more:
        copy.start()
    top[...] = gather(order[2], copies)
    for _, copy in started:
        copy.wait_send()
    for copy in halos + more:
        copy.wait()


def project(u, vn, va, vb, kin, b1h, ich):
    a = u[4] + kin * u[0] - vn * u[1] - va * u[2] - vb * u[3]
    a = b1h * a
    b = (vn * u[0] - u[1]) * ich
    return [a + b, u[2] - va * u[0], u[3] - vb * u[0], u[0] - (a + a), a - b]


def nonlinear(e1, e2, e3, f0, f1):
    f2 = e3 - (f1 + e2)
    q0 = 1.0 / ((K13 * (e1 * e1) + EPS) + f0 * f0)
    q1 = 1.0 / ((K13 * (e2 * e2) + EPS) + f1 * f1)
    q2 = 1.0 / ((K13 * (e3 * e3) + EPS) + f2 * f2)
    w0 = q0 * q0
    w2 = 3.0 * (q2 * q2)
    n0 = e1 - e2
    return (w0 * (n0 + n0) + w2 * (e2 - e3)) / (w0 + w2 + 6.0 * (q1 * q1))


def flux_sweep(direction, slots, lane_rows, quarter, q, p, m, f6, ep, em, hp, hm, flux):
    order = ORDERS[direction]

    def at(ref, c, j):
        return ref[c, pl.ds(pl.multiple_of(8 * j, 8), 8), :]

    def put(ref, c, j, value):
        ref[c, pl.ds(pl.multiple_of(8 * j, 8), 8), :] = value

    r = lane_rows

    def cell(j, _):
        s = [at(q, order[c], j) for c in range(5)]
        inv = 1.0 / s[0]
        vq = s[1] * (0.25 * inv)
        pq = 0.25 * (GAMMA - 1.0) * (s[4] - (0.5 * inv) * (s[1] * s[1] + s[2] * s[2] + s[3] * s[3]))
        f = [0.25 * s[1], s[1] * vq + pq, s[2] * vq, s[3] * vq, s[4] * vq + 4.0 * (pq * vq)]
        for c in range(5):
            sq = quarter * s[c]
            put(p, c, j, f[c] + sq)
            put(m, c, j, f[c] - sq)
            put(f6, c, j, 6.0 * f[c])
        return 0

    lax.fori_loop(0, (slots + 6) * r, cell, 0, unroll=2)

    def differ(i, _):
        j = i + r
        for c in range(5):
            for src, e, h in ((p, ep, hp), (m, em, hm)):
                low, mid, high = at(src, c, j - r), at(src, c, j), at(src, c, j + r)
                below = mid - low
                put(e, c, j, (high - mid) - below)
                put(h, c, j, below + below)
        return 0

    lax.fori_loop(0, (slots + 4) * r, differ, 0, unroll=2)

    def face(j, _):
        mean = [at(q, order[c], j + 2 * r) + at(q, order[c], j + 3 * r) for c in range(5)]
        inv = 1.0 / mean[0]
        vn, va, vb = mean[1] * inv, mean[2] * inv, mean[3] * inv
        kin = 0.5 * (vn * vn + va * va + vb * vb)
        c2 = GAMMA * (GAMMA - 1.0) * (mean[4] * inv - kin)
        ic = lax.rsqrt(c2)
        b1h = (0.5 * (GAMMA - 1.0)) * (ic * ic)
        ich = 0.5 * ic
        args = (vn, va, vb, kin, b1h, ich)
        e2p = [at(ep, c, j + 2 * r) for c in range(5)]
        e1, e3 = ([at(ep, c, j + k * r) for c in range(5)] for k in (1, 3))
        h = [at(hp, c, j + 2 * r) for c in range(5)]
        e1, e2, e3, h = (project(u, *args) for u in (e1, e2p, e3, h))
        n = [nonlinear(e1[k], e2[k], e3[k], h[k] + e1[k], h[k] + e2[k]) for k in range(5)]
        e2m = [at(em, c, j + 3 * r) for c in range(5)]
        e1, e3 = ([at(em, c, j + k * r) for c in range(5)] for k in (4, 2))
        h = [at(hm, c, j + 4 * r) for c in range(5)]
        e1, e2, e3, h = (project(u, *args) for u in (e1, e2m, e3, h))
        n = [n[k] + nonlinear(e1[k], e2[k], e3[k], e1[k] - h[k], e2[k] - h[k]) for k in range(5)]
        d = (c2 * ic) * (n[4] - n[0])
        s15 = n[0] + n[4]
        s = s15 + n[3]
        enthalpy = (1.0 / (GAMMA - 1.0)) * c2 + kin
        out = [
            s,
            vn * s + d,
            va * s + n[1],
            vb * s + n[2],
            enthalpy * s15 + vn * d + va * n[1] + vb * n[2] + kin * n[3],
        ]
        for c in range(5):
            linear = at(f6, c, j + 2 * r) + at(f6, c, j + 3 * r)
            linear = linear - at(ep, c, j + 2 * r) - at(em, c, j + 3 * r)
            put(flux, order[c], j, linear + out[c])
        return 0

    lax.fori_loop(0, (slots + 1) * r, face, 0)


def advance_kernel(cells, shape, cons, xh, yh, zh, zt, top, out, q, p, m, f6, ep, em, hp, hm, fx, fy, fz):
    lx, ly, lz = shape
    rows = lx * ly
    groups = rows // LANES
    blocks = 8 // groups
    inner = lz // blocks
    speeds = []
    for d in range(3):
        best = jnp.max(jnp.max(top[pl.ds(8 * d, 8), :], axis=0, keepdims=True), axis=1, keepdims=True)
        speeds.append(jnp.broadcast_to(best, (8, LANES)))
    step = COURANT / (speeds[0] * cells[0] + speeds[1] * cells[1] + speeds[2] * cells[2])
    work = (q, p, m, f6, ep, em, hp, hm)

    edge = 3 * ly
    q[:, pl.ds(0, edge), :] = xh[0]
    q[:, pl.ds(edge, rows), :] = cons[...]
    q[:, pl.ds(edge + rows, edge), :] = xh[1]
    flux_sweep(0, lx, ly // 8, 0.25 * speeds[0], *work, fx)

    edge = 3 * lx
    q[:, pl.ds(0, edge), :] = yh[0]
    for c in range(5):
        for y in range(ly):
            q[c, pl.ds(edge + y * lx, lx), :] = cons[c, pl.ds(y, lx, stride=ly), :]
    q[:, pl.ds(edge + rows, edge), :] = yh[1]
    flux_sweep(1, ly, lx // 8, 0.25 * speeds[1], *work, fy)

    size = inner * 8
    q[:, pl.ds(24, size), :] = zt[...]
    for c in range(5):
        for k in range(3):
            low, high = 8 * k, 24 + size + 8 * k
            q[c, low:low + groups, :] = zh[0, c, k]
            q[c, low + groups:low + 8, :] = zt[c, size - 24 + 8 * k:size - 16 + 8 * k - groups, :]
            q[c, high:high + 8 - groups, :] = zt[c, 8 * k + groups:8 * k + 8, :]
            q[c, high + 8 - groups:high + 8, :] = zh[1, c, k]
    flux_sweep(2, inner, 1, 0.25 * speeds[2], *work, fz)

    scale = [step * (cells[d] / 3.0) for d in range(3)]
    for c in range(5):
        def drop(j, _):
            here = pl.ds(pl.multiple_of(8 * j, 8), 8)
            fz[c, here, :] = scale[2] * (fz[c, here, :] - fz[c, pl.ds(pl.multiple_of(8 * j + 8, 8), 8), :])
            return 0

        lax.fori_loop(0, inner, drop, 0, unroll=4)
        for y in range(ly):
            for h in range(lx // 8):
                here = fy[c, pl.ds(y * lx + 8 * h, 8), :]
                there = fy[c, pl.ds((y + 1) * lx + 8 * h, 8), :]
                out[c, pl.ds(8 * h * ly + y, 8, stride=ly), :] = scale[1] * (here - there)
        for g in range(groups):
            parts = [fz[c, pl.ds(b * groups + g, inner, stride=8), :] for b in range(blocks)]
            turned = jnp.transpose(jnp.concatenate(parts, axis=0))
            for t in range(LANES // 8):
                at = g * LANES + 8 * t
                here = pl.ds(at, 8)
                along_x = scale[0] * (fx[c, here, :] - fx[c, pl.ds(at + ly, 8), :])
                out[c, here, :] = cons[c, here, :] + ((out[c, here, :] + along_x) + turned[8 * t:8 * t + 8])


def solution(mesh):
    sizes = [mesh.shape[axis] for axis in AXES]

    def per_device(conserved):
        _, lx, ly, lz = conserved.shape
        shape = (lx, ly, lz)
        cells = [float(n * s) for n, s in zip(shape, sizes)]
        rows = lx * ly
        groups = rows // LANES
        inner = lz * groups // 8
        assert lz == LANES and rows % LANES == 0 and 8 % groups == 0 and lx % 8 == 0 and ly % 8 == 0
        flat = conserved.reshape(5, rows, lz)
        vmem = pl.BlockSpec(memory_space=pltpu.VMEM)
        total = sum(s - 1 for s in sizes)
        f32 = jnp.float32
        xh, yh, zh, zt, top = pl.pallas_call(
            functools.partial(exchange_kernel, sizes, shape),
            name="exchange",
            out_shape=[
                jax.ShapeDtypeStruct((2, 5, 3 * ly, lz), f32),
                jax.ShapeDtypeStruct((2, 5, 3 * lx, lz), f32),
                jax.ShapeDtypeStruct((2, 5, 3, groups, LANES), f32),
                jax.ShapeDtypeStruct((5, inner * 8, LANES), f32),
                jax.ShapeDtypeStruct((24, LANES), f32),
            ],
            in_specs=[vmem],
            out_specs=[vmem] * 5,
            scratch_shapes=[
                pltpu.VMEM((2, 5, 3 * lx, lz), f32),
                pltpu.VMEM((2, 5, 3, groups, LANES), f32),
                pltpu.VMEM((3, 24, LANES), f32),
                pltpu.VMEM((total, 24, LANES), f32),
                pltpu.SemaphoreType.DMA((6,)),
                pltpu.SemaphoreType.DMA((6,)),
                pltpu.SemaphoreType.DMA((total,)),
                pltpu.SemaphoreType.DMA((total,)),
            ],
            compiler_params=pltpu.CompilerParams(collective_id=0, has_side_effects=True),
        )(flat)
        padded = max((lx + 6) * ly, (ly + 6) * lx, (inner + 6) * 8)
        work = pltpu.VMEM((5, padded, LANES), f32)
        out = pl.pallas_call(
            functools.partial(advance_kernel, cells, shape),
            name="advance",
            out_shape=jax.ShapeDtypeStruct((5, rows, lz), f32),
            in_specs=[vmem] * 6,
            out_specs=vmem,
            scratch_shapes=[work] * 8 + [
                pltpu.VMEM((5, (lx + 1) * ly, LANES), f32),
                pltpu.VMEM((5, (ly + 1) * lx, LANES), f32),
                pltpu.VMEM((5, (inner + 1) * 8, LANES), f32),
            ],
        )(flat, xh, yh, zh, zt, top)
        return out.reshape(conserved.shape)

    return jax.shard_map(
        per_device,
        mesh=mesh,
        in_specs=(P(None, "gx", "gy", "gz"),),
        out_specs=P(None, "gx", "gy", "gz"),
        check_vma=False,
    )
```

```python
import functools

import jax
import jax.numpy as jnp
from jax import lax
from jax.experimental import pallas as pl
from jax.experimental.pallas import tpu as pltpu
from jax.sharding import PartitionSpec as P

GAMMA = 1.4
EPS = 1e-06
COURANT = 0.4
K13 = 13.0 / 3.0
MESH = pl.DeviceIdType.MESH
AXES = ("gx", "gy", "gz")
ORDERS = ([0, 1, 2, 3, 4], [0, 2, 1, 3, 4], [0, 3, 1, 2, 4])
LANES = 128


def project(u, vn, va, vb, kin, b1h, ich):
    a = u[4] + kin * u[0] - vn * u[1] - va * u[2] - vb * u[3]
    a = b1h * a
    b = (vn * u[0] - u[1]) * ich
    return [a + b, u[2] - va * u[0], u[3] - vb * u[0], u[0] - (a + a), a - b]


def nonlinear(e1, e2, e3, f0, f1):
    f2 = e3 - (f1 + e2)
    q0 = 1.0 / ((K13 * (e1 * e1) + EPS) + f0 * f0)
    q1 = 1.0 / ((K13 * (e2 * e2) + EPS) + f1 * f1)
    q2 = 1.0 / ((K13 * (e3 * e3) + EPS) + f2 * f2)
    w0 = q0 * q0
    w2 = 3.0 * (q2 * q2)
    n0 = e1 - e2
    return (w0 * (n0 + n0) + w2 * (e2 - e3)) / (w0 + w2 + 6.0 * (q1 * q1))


def flux_sweep(direction, slots, lane_rows, quarter, q, p, m, f6, ep, em, hp, hm, flux):
    order = ORDERS[direction]

    def at(ref, c, j):
        return ref[c, pl.ds(pl.multiple_of(8 * j, 8), 8), :]

    def put(ref, c, j, value):
        ref[c, pl.ds(pl.multiple_of(8 * j, 8), 8), :] = value

    r = lane_rows

    def cell(j, _):
        s = [at(q, order[c], j) for c in range(5)]
        inv = 1.0 / s[0]
        vq = s[1] * (0.25 * inv)
        pq = 0.25 * (GAMMA - 1.0) * (s[4] - (0.5 * inv) * (s[1] * s[1] + s[2] * s[2] + s[3] * s[3]))
        f = [0.25 * s[1], s[1] * vq + pq, s[2] * vq, s[3] * vq, s[4] * vq + 4.0 * (pq * vq)]
        for c in range(5):
            sq = quarter * s[c]
            put(p, c, j, f[c] + sq)
            put(m, c, j, f[c] - sq)
            put(f6, c, j, 6.0 * f[c])
        return 0

    lax.fori_loop(0, (slots + 6) * r, cell, 0, unroll=2)

    def differ(i, _):
        j = i + r
        for c in range(5):
            for src, e, h in ((p, ep, hp), (m, em, hm)):
                low, mid, high = at(src, c, j - r), at(src, c, j), at(src, c, j + r)
                below = mid - low
                put(e, c, j, (high - mid) - below)
                put(h, c, j, below + below)
        return 0

    lax.fori_loop(0, (slots + 4) * r, differ, 0, unroll=2)

    def face(j, _):
        mean = [at(q, order[c], j + 2 * r) + at(q, order[c], j + 3 * r) for c in range(5)]
        inv = 1.0 / mean[0]
        vn, va, vb = mean[1] * inv, mean[2] * inv, mean[3] * inv
        kin = 0.5 * (vn * vn + va * va + vb * vb)
        c2 = GAMMA * (GAMMA - 1.0) * (mean[4] * inv - kin)
        ic = lax.rsqrt(c2)
        b1h = (0.5 * (GAMMA - 1.0)) * (ic * ic)
        ich = 0.5 * ic
        args = (vn, va, vb, kin, b1h, ich)
        e2p = [at(ep, c, j + 2 * r) for c in range(5)]
        e1, e3 = ([at(ep, c, j + k * r) for c in range(5)] for k in (1, 3))
        h = [at(hp, c, j + 2 * r) for c in range(5)]
        e1, e2, e3, h = (project(u, *args) for u in (e1, e2p, e3, h))
        n = [nonlinear(e1[k], e2[k], e3[k], h[k] + e1[k], h[k] + e2[k]) for k in range(5)]
        e2m = [at(em, c, j + 3 * r) for c in range(5)]
        e1, e3 = ([at(em, c, j + k * r) for c in range(5)] for k in (4, 2))
        h = [at(hm, c, j + 4 * r) for c in range(5)]
        e1, e2, e3, h = (project(u, *args) for u in (e1, e2m, e3, h))
        n = [n[k] + nonlinear(e1[k], e2[k], e3[k], e1[k] - h[k], e2[k] - h[k]) for k in range(5)]
        d = (c2 * ic) * (n[4] - n[0])
        s15 = n[0] + n[4]
        s = s15 + n[3]
        enthalpy = (1.0 / (GAMMA - 1.0)) * c2 + kin
        out = [
            s,
            vn * s + d,
            va * s + n[1],
            vb * s + n[2],
            enthalpy * s15 + vn * d + va * n[1] + vb * n[2] + kin * n[3],
        ]
        for c in range(5):
            linear = at(f6, c, j + 2 * r) + at(f6, c, j + 3 * r)
            linear = linear - at(ep, c, j + 2 * r) - at(em, c, j + 3 * r)
            put(flux, order[c], j, linear + out[c])
        return 0

    lax.fori_loop(0, (slots + 1) * r, face, 0)


def section_kernel(
    sizes, cells, shape, cons_hbm, out_hbm, cons, out, qx, qy, qz, xh, yh, zh, ysend, zsend, mine, theirs,
    p, m, f6, ep, em, hp, hm, fx, fy, fz, halo_send, halo_recv, max_send, max_recv, load_sem, store_sem,
):
    lx, ly, lz = shape
    rows = lx * ly
    groups = rows // LANES
    blocks = 8 // groups
    inner = lz // blocks
    load = pltpu.make_async_copy(cons_hbm, cons, load_sem)
    load.start()
    peers = []
    for axis, size in zip(AXES, sizes):
        me = lax.axis_index(axis)
        peers.append([{axis: lax.rem(me + k, size)} for k in range(1, size)])
    barrier = pltpu.get_barrier_semaphore()
    count = 0
    for axis_peers in peers:
        for peer in axis_peers:
            pl.semaphore_signal(barrier, inc=1, device_id=peer, device_id_type=MESH)
            count += 1
    load.wait()

    best = [None] * 3
    for j in range(rows // 8):
        q = [cons[c, pl.ds(8 * j, 8), :] for c in range(5)]
        inv = 1.0 / q[0]
        vel = [q[d] * inv for d in (1, 2, 3)]
        kinetic = 0.5 * (vel[0] * vel[0] + vel[1] * vel[1] + vel[2] * vel[2])
        sound = jnp.sqrt((GAMMA * (GAMMA - 1.0)) * (q[4] * inv - kinetic))
        for d in range(3):
            value = jnp.abs(vel[d]) + sound
            best[d] = value if best[d] is None else jnp.maximum(best[d], value)
    for d in range(3):
        mine[0, pl.ds(d, 1), :] = jnp.max(best[d], axis=0, keepdims=True)
    mine[0, pl.ds(3, 5), :] = jnp.zeros((5, LANES), jnp.float32)

    for c in range(5):
        for k in range(3):
            ysend[0, c, pl.ds(k * lx, lx), :] = cons[c, pl.ds(ly - 3 + k, lx, stride=ly), :]
            ysend[1, c, pl.ds(k * lx, lx), :] = cons[c, pl.ds(k, lx, stride=ly), :]

    def halo(slot, src, dst, axis, size, up):
        me = lax.axis_index(axis)
        target = lax.rem(me + (1 if up else size - 1), size)
        return pltpu.make_async_remote_copy(
            src_ref=src, dst_ref=dst, send_sem=halo_send.at[slot], recv_sem=halo_recv.at[slot],
            device_id={axis: target}, device_id_type=MESH,
        )

    def spread(place, stage):
        size = sizes[stage]
        copies = []
        for k in range(size - 1):
            slot = sum(s - 1 for s in sizes[:stage]) + k
            copy = pltpu.make_async_remote_copy(
                src_ref=mine.at[place], dst_ref=theirs.at[slot],
                send_sem=max_send.at[slot], recv_sem=max_recv.at[slot],
                device_id=peers[stage][k], device_id_type=MESH,
            )
            copy.start()
            copies.append((slot, copy))
        return copies

    def gather(place, copies):
        value = mine[place]
        for slot, copy in copies:
            copy.wait_recv()
            value = jnp.maximum(value, theirs[slot])
        return value

    pl.semaphore_wait(barrier, count)
    first = spread(0, 0)
    edge = 3 * ly
    along_x = [
        halo(0, cons.at[:, pl.ds(rows - edge, edge), :], xh.at[0], "gx", sizes[0], True),
        halo(1, cons.at[:, pl.ds(0, edge), :], xh.at[1], "gx", sizes[0], False),
    ]
    along_y = [
        halo(2, ysend.at[0], yh.at[0], "gy", sizes[1], True),
        halo(3, ysend.at[1], yh.at[1], "gy", sizes[1], False),
    ]
    along_z = [
        halo(4, zsend.at[0], zh.at[0], "gz", sizes[2], True),
        halo(5, zsend.at[1], zh.at[1], "gz", sizes[2], False),
    ]
    for copy in along_y + along_x:
        copy.start()

    for c in range(5):
        for g in range(groups):
            turned = jnp.transpose(cons[c, pl.ds(g * LANES, LANES), :])
            for b in range(blocks):
                qz[c, pl.ds(24 + b * groups + g, inner, stride=8), :] = turned[b * inner:(b + 1) * inner]
            for k in range(3):
                zsend[0, c, k, g:g + 1, :] = turned[lz - 3 + k:lz - 2 + k]
                zsend[1, c, k, g:g + 1, :] = turned[k:k + 1]

    mine[1] = gather(0, first)
    second = spread(1, 2)
    for copy in along_z:
        copy.start()

    y_edge = 3 * lx
    for c in range(5):
        for y in range(ly):
            qy[c, pl.ds(y_edge + y * lx, lx), :] = cons[c, pl.ds(y, lx, stride=ly), :]

    mine[2] = gather(1, second)
    third = spread(2, 1)
    for copy in along_y:
        copy.wait()
    qy[:, pl.ds(0, y_edge), :] = yh[0]
    qy[:, pl.ds(y_edge + rows, y_edge), :] = yh[1]
    qx[:, pl.ds(edge, rows), :] = cons[...]
    top = gather(2, third)
    for _, copy in first + second + third:
        copy.wait_send()

    speeds = []
    for d in range(3):
        largest = jnp.max(top[d:d + 1], axis=1, keepdims=True)
        speeds.append(jnp.broadcast_to(largest, (8, LANES)))
    step = COURANT / (speeds[0] * cells[0] + speeds[1] * cells[1] + speeds[2] * cells[2])
    work = (p, m, f6, ep, em, hp, hm)

    flux_sweep(1, ly, lx // 8, 0.25 * speeds[1], qy, *work, fy)

    for copy in along_z:
        copy.wait()
    size = inner * 8
    for c in range(5):
        for k in range(3):
            low, high = 8 * k, 24 + size + 8 * k
            qz[c, low:low + groups, :] = zh[0, c, k]
            qz[c, low + groups:low + 8, :] = qz[c, size + 8 * k:size + 8 + 8 * k - groups, :]
            qz[c, high:high + 8 - groups, :] = qz[c, 24 + 8 * k + groups:32 + 8 * k, :]
            qz[c, high + 8 - groups:high + 8, :] = zh[1, c, k]
    flux_sweep(2, inner, 1, 0.25 * speeds[2], qz, *work, fz)

    for copy in along_x:
        copy.wait()
    qx[:, pl.ds(0, edge), :] = xh[0]
    qx[:, pl.ds(edge + rows, edge), :] = xh[1]
    flux_sweep(0, lx, ly // 8, 0.25 * speeds[0], qx, *work, fx)

    scale = [step * (cells[d] / 3.0) for d in range(3)]
    stores = []
    for c in range(5):
        def drop(j, _):
            here = pl.ds(pl.multiple_of(8 * j, 8), 8)
            fz[c, here, :] = scale[2] * (fz[c, here, :] - fz[c, pl.ds(pl.multiple_of(8 * j + 8, 8), 8), :])
            return 0

        lax.fori_loop(0, inner, drop, 0, unroll=8)
        for y in range(ly):
            for h in range(lx // 8):
                here = fy[c, pl.ds(y * lx + 8 * h, 8), :]
                there = fy[c, pl.ds((y + 1) * lx + 8 * h, 8), :]
                out[c, pl.ds(8 * h * ly + y, 8, stride=ly), :] = scale[1] * (here - there)
        for g in range(groups):
            parts = [fz[c, pl.ds(b * groups + g, inner, stride=8), :] for b in range(blocks)]
            turned = jnp.transpose(jnp.concatenate(parts, axis=0))
            for t in range(LANES // 8):
                at = g * LANES + 8 * t
                here = pl.ds(at, 8)
                change = scale[0] * (fx[c, here, :] - fx[c, pl.ds(at + ly, 8), :])
                out[c, here, :] = cons[c, here, :] + ((out[c, here, :] + change) + turned[8 * t:8 * t + 8])
        stores.append(pltpu.make_async_copy(out.at[c], out_hbm.at[c], store_sem.at[c]))
        if c > 0:
            stores[c - 1].start()
    stores[-1].start()
    for store in stores:
        store.wait()


def solution(mesh):
    sizes = [mesh.shape[axis] for axis in AXES]

    def per_device(conserved):
        _, lx, ly, lz = conserved.shape
        shape = (lx, ly, lz)
        cells = [float(n * s) for n, s in zip(shape, sizes)]
        rows = lx * ly
        groups = rows // LANES
        inner = lz * groups // 8
        assert lz == LANES and rows % LANES == 0 and 8 % groups == 0 and lx % 8 == 0 and ly % 8 == 0
        total = sum(s - 1 for s in sizes)

        def vmem(*dims):
            return pltpu.VMEM(dims, jnp.float32)

        padded = max((lx + 6) * ly, (ly + 6) * lx, (inner + 6) * 8)
        out = pl.pallas_call(
            functools.partial(section_kernel, sizes, cells, shape),
            name="section",
            out_shape=jax.ShapeDtypeStruct((5, rows, lz), jnp.float32),
            in_specs=[pl.BlockSpec(memory_space=pl.ANY)],
            out_specs=pl.BlockSpec(memory_space=pl.ANY),
            scratch_shapes=[
                vmem(5, rows, lz),
                vmem(5, rows, lz),
                vmem(5, padded, LANES),
                vmem(5, padded, LANES),
                vmem(5, padded, LANES),
                vmem(2, 5, 3 * ly, lz),
                vmem(2, 5, 3 * lx, lz),
                vmem(2, 5, 3, groups, LANES),
                vmem(2, 5, 3 * lx, lz),
                vmem(2, 5, 3, groups, LANES),
                vmem(3, 8, LANES),
                vmem(total, 8, LANES),
            ] + [vmem(5, padded, LANES)] * 7 + [
                vmem(5, (lx + 1) * ly, LANES),
                vmem(5, (ly + 1) * lx, LANES),
                vmem(5, (inner + 1) * 8, LANES),
                pltpu.SemaphoreType.DMA((6,)),
                pltpu.SemaphoreType.DMA((6,)),
                pltpu.SemaphoreType.DMA((total,)),
                pltpu.SemaphoreType.DMA((total,)),
                pltpu.SemaphoreType.DMA,
                pltpu.SemaphoreType.DMA((5,)),
            ],
            compiler_params=pltpu.CompilerParams(collective_id=0, has_side_effects=True),
        )(conserved.reshape(5, rows, lz))
        return out.reshape(conserved.shape)

    return jax.shard_map(
        per_device,
        mesh=mesh,
        in_specs=(P(None, "gx", "gy", "gz"),),
        out_specs=P(None, "gx", "gy", "gz"),
        check_vma=False,
    )
```
